32 devices in a mesh: dp: 8 (over z, y), mp: 4 (over x, core).
Axes of the slice: x: 2, y: 2, z: 4, core: 2. Of those that a mesh axis runs over, the one named last changes fastest.
Arguments:
- image_tokens: bfloat16 [8, 192, 3072], P('dp'), may hold values from -6 to 6
- text_tokens: bfloat16 [8, 64, 3072], P('dp'), may hold values from -6 to 6
- null_prompt: bfloat16 [64, 3072], replicated, may hold values from -6 to 6
- drop_flags: int32 [8], P('dp'), may hold values 0 or 1
- time_index: int32 [8], P('dp'), may hold values from 0 to 31
- modulation: float32 [32, 3, 3072], replicated, may hold values from -3 to 3
- w_up: bfloat16 [3072, 12288], P('dp', 'mp'), may hold values from -0.109375 to 0.109375
- w_down: bfloat16 [12288, 3072], P('mp', 'dp'), may hold values from -0.0546875 to 0.0546875
- d_output: bfloat16 [8, 256, 3072], P('dp'), may hold values from -6 to 6
Outputs:
- block_out: bfloat16 [8, 256, 3072], P('dp')
- d_tokens: bfloat16 [8, 256, 3072], P('dp')
- grad_up: float32 [3072, 12288], P('dp', 'mp')
- grad_down: float32 [12288, 3072], P('mp', 'dp')
- grad_null: float32 [64, 3072], replicated
The draws below stay inside these ranges and needn't reach their ends.
All inputs are finite; a program needn't handle non-finite values. No bound on the sum of `drop_flags` on one device may be relied on, other than what follows from the above.
Results may differ from the reference program's by a relative error of at most 0.017.
Values may be sent and summed in bfloat16 or wider, within the bound.
A program may use at most 128 MiB of HBM per device.

```python
import jax
import jax.numpy as jnp
from jax import lax

D = 3072
FF = 12288
L_IMG = 192
L_TXT = 64
NT = 32
B = 8
L = 256
N_MP = 4


def touch_ends(values, stream_key, low, largest):
    extent = values.shape
    place = [jax.random.randint(jax.random.fold_in(stream_key, axis), (), 0, extent[axis]) for axis in range(len(extent))]
    values = values.at[tuple(place)].set(low)
    longest = extent.index(max(extent))
    place[longest] = (place[longest] + 1) % extent[longest]
    return values.at[tuple(place)].set(largest)


def block_levels(key, shape, pieces, low, largest):
    gain = 1.0
    for axis_at, shards_of in pieces:
        heights = jax.random.uniform(jax.random.fold_in(jax.random.fold_in(key, 6), axis_at), (shards_of,), jnp.float32, low / len(pieces), largest / len(pieces))
        gain = gain * jnp.repeat(jnp.exp(heights), shape[axis_at] // shards_of).reshape((-1,) + (1,) * (len(shape) - 1 - axis_at))
    return gain


def gaussian(rng, dims, scale, most, shards=(), held_as=jnp.bfloat16):
    result = jax.random.normal(rng, dims, jnp.float32) * scale
    if len(shards) > 0:
        result = block_levels(rng, dims, shards, -0.22, 0.18) * result
    return jnp.clip(result, min=-most, max=most).astype(held_as)


def setup_inputs(seed: int = 0) -> dict:
    key_list = jax.random.split(jax.random.key(seed), 10)
    return {
        "image_tokens": gaussian(key_list[0], (B, L_IMG, D), 1.0, 6.0, ((0, 8),)),
        "text_tokens": gaussian(key_list[1], (B, L_TXT, D), 1.0, 6.0, ((0, 8),)),
        "null_prompt": gaussian(key_list[2], (L_TXT, D), 1.0, 6.0),
        "drop_flags": touch_ends((jax.random.randint(key_list[3], (B,), 0, 2) < 1).astype(jnp.int32), jax.random.fold_in(key_list[3], 1), 0, 1),
        "time_index": touch_ends(jax.random.randint(key_list[4], (B,), 0, NT), jax.random.fold_in(key_list[4], 1), 0, NT - 1).astype(jnp.int32),
        "modulation": gaussian(key_list[5], (NT, 3, D), 0.5, 3.0, (), jnp.float32),
        "w_up": gaussian(key_list[6], (D, FF), D ** -0.5, 0.109375, ((0, 8), (1, 4))),
        "w_down": gaussian(key_list[7], (FF, D), FF ** -0.5, 0.0546875, ((0, 4), (1, 8))),
        "d_output": gaussian(key_list[8], (B, L, D), 1.0, 6.0, ((0, 8),)),
    }


EPS = 1e-06

def gelu_tanh(values):
    return jax.nn.gelu(values, approximate=True)

def reference(image_tokens, text_tokens, null_prompt, drop_flags, time_index, modulation, w_up, w_down, d_output):
    dropped = drop_flags == 1
    text_in = jnp.where(dropped[:, None, None], null_prompt[None], text_tokens)
    joined = jnp.concatenate([text_in, image_tokens], axis=1)
    levels = jnp.arange(modulation.shape[0], dtype=jnp.int32)
    indicator_matrix = (time_index[:, None] == levels[None, :]).astype(jnp.float32)
    modulation_vectors = jnp.einsum('yi,imr->ymr', indicator_matrix, modulation.astype(jnp.float32), precision=lax.Precision.HIGHEST)
    shift_modulation = modulation_vectors[:, 0][:, None]
    scale_mod = modulation_vectors[:, 1][:, None]
    gate_mod = modulation_vectors[:, 2][:, None]
    batch, length, width = joined.shape
    joined32 = joined.astype(jnp.float32)
    centred = joined32 - lax.optimization_barrier(jnp.mean(joined32, axis=-1, keepdims=True))
    inv_std = lax.rsqrt(lax.optimization_barrier(jnp.mean(centred * centred, axis=-1, keepdims=True)) + EPS)
    normed = centred * inv_std
    mod_in = (normed * (1.0 + scale_mod) + shift_modulation).astype(jnp.bfloat16)
    flat_in = mod_in.reshape(batch * length, width)
    preactivation_rows = jnp.dot(flat_in, w_up, preferred_element_type=jnp.float32)
    hidden = gelu_tanh(preactivation_rows).astype(jnp.bfloat16)
    per_part = w_up.shape[1] // N_MP
    block_ids = jnp.arange(N_MP, dtype=jnp.int32)

    def add_branch(total, block_no):
        start = (block_no * per_part).astype(jnp.int32)
        cols = lax.dynamic_slice_in_dim(hidden, start, per_part, 1)
        rows_w = lax.dynamic_slice_in_dim(w_down, start, per_part, 0)
        part = jnp.dot(cols, rows_w, preferred_element_type=jnp.float32).astype(jnp.bfloat16)
        part = lax.optimization_barrier(part)
        return (total + part.astype(jnp.float32), None)
    branch, _ = lax.scan(add_branch, jnp.zeros((batch * length, width), jnp.float32), block_ids)
    branch = branch.reshape(batch, length, width)
    block_out = (joined32 + gate_mod * branch).astype(jnp.bfloat16)
    d_out32 = d_output.astype(jnp.float32)
    d_branch = (d_out32 * gate_mod).astype(jnp.bfloat16).reshape(batch * length, width)
    hidden_gradient = jnp.dot(d_branch, w_down.T, preferred_element_type=jnp.float32)
    _, gelu_back = jax.vjp(gelu_tanh, preactivation_rows)
    d_pre = gelu_back(hidden_gradient)[0].astype(jnp.bfloat16)
    grad_down = jnp.dot(hidden.T, d_branch, preferred_element_type=jnp.float32)
    grad_up = jnp.dot(flat_in.T, d_pre, preferred_element_type=jnp.float32)

    def add_input(total, block_no):
        start = (block_no * per_part).astype(jnp.int32)
        cols = lax.dynamic_slice_in_dim(d_pre, start, per_part, 1)
        wcols = lax.dynamic_slice_in_dim(w_up, start, per_part, 1)
        part = jnp.dot(cols, wcols.T, preferred_element_type=jnp.float32).astype(jnp.bfloat16)
        part = lax.optimization_barrier(part)
        return (total + part.astype(jnp.float32), None)
    d_mod, _ = lax.scan(add_input, jnp.zeros((batch * length, width), jnp.float32), block_ids)
    d_normed = d_mod.reshape(batch, length, width) * (1.0 + scale_mod)
    d_full = d_out32 + inv_std * (d_normed - lax.optimization_barrier(jnp.mean(d_normed, axis=-1, keepdims=True)) - normed * lax.optimization_barrier(jnp.mean(d_normed * normed, axis=-1, keepdims=True)))
    grad_null = lax.optimization_barrier(jnp.sum(jnp.where(dropped[:, None, None], d_full[:, :L_TXT], jnp.float32(0.0)), axis=0))
    return (block_out, d_full.astype(jnp.bfloat16), grad_up, grad_down, grad_null)
```

```python
import functools

import jax
import jax.numpy as jnp
from jax import lax
from jax.sharding import PartitionSpec as P

EPS = 1e-06
BF16 = jnp.bfloat16
F32 = jnp.float32


def gelu_tanh(values):
    return jax.nn.gelu(values, approximate=True)


def dot(left, right, dims):
    return lax.dot_general(left, right, (dims, ((), ())), preferred_element_type=F32)


def swap(values, axis, size, bit):
    return lax.ppermute(values, axis, [(i, i ^ bit) for i in range(size)])


def shards(
    dp,
    mp,
    image_tokens,
    text_tokens,
    null_prompt,
    drop_flags,
    time_index,
    modulation,
    w_up,
    w_down,
    d_output,
):
    lines = [list(range(parity, dp, 2)) for parity in range(2)]
    per_line = dp // 2
    bits = []
    bit = 1
    while bit < mp:
        bits.append(bit)
        bit *= 2

    d_rows, ff_m = w_up.shape
    f = ff_m // dp
    width = d_rows * dp

    up_own = lax.all_to_all(
        w_up.reshape(d_rows, dp, f).transpose(1, 0, 2), "dp", 0, 0, tiled=True
    ).reshape(width, f)
    down_own = (
        lax.all_to_all(w_down.reshape(dp, f, d_rows), "dp", 0, 0, tiled=True)
        .transpose(1, 0, 2)
        .reshape(f, width)
    )
    up_other = swap(up_own, "dp", dp, 1)
    down_other = swap(down_own, "dp", dp, 1)

    m = lax.axis_index("mp")
    n_text = text_tokens.shape[1] // mp
    n_image = image_tokens.shape[1] // mp
    all_text = text_tokens.shape[1]

    def share(text_part, image_part):
        t = lax.dynamic_slice_in_dim(text_part, m * n_text, n_text, 0)
        i = lax.dynamic_slice_in_dim(image_part, m * n_image, n_image, 0)
        return jnp.concatenate([t, i], axis=0)

    dropped = drop_flags[0] == 1
    joined32 = share(
        jnp.where(dropped, null_prompt, text_tokens[0]), image_tokens[0]
    ).astype(F32)
    d_out32 = share(d_output[0, :all_text], d_output[0, all_text:]).astype(F32)
    level = lax.dynamic_index_in_dim(modulation, time_index[0], 0, keepdims=False)
    shift, scale, gate = level[0][None], level[1][None], level[2][None]
    centred = joined32 - jnp.mean(joined32, axis=-1, keepdims=True)
    inv_std = lax.rsqrt(jnp.mean(centred * centred, axis=-1, keepdims=True) + EPS)
    normed = centred * inv_std
    mod_in = (normed * (1.0 + scale) + shift).astype(BF16)
    d_branch = (d_out32 * gate).astype(BF16)

    def gather(rows):
        rows = lax.all_gather(rows, "dp", axis=0, tiled=True, axis_index_groups=lines)
        for b in reversed(bits):
            rows = jnp.concatenate([rows, swap(rows, "mp", mp, b)], axis=0)
        return rows

    def scatter(own, other, block_own, block_other, contract):
        def product(rows):
            return dot(own[rows], block_own, contract) + dot(other[rows], block_other, contract)

        half = own.shape[0] // 2
        sent = swap(product(slice(half, None)).astype(BF16), "mp", mp, bits[0])
        total = product(slice(0, half)) + sent.astype(F32)
        for b in bits[1:]:
            half = total.shape[0] // 2
            total = total[:half] + swap(total[half:].astype(BF16), "mp", mp, b).astype(F32)
        parts = lax.all_to_all(
            total.astype(BF16).reshape(per_line, -1, width),
            "dp",
            0,
            0,
            tiled=True,
            axis_index_groups=lines,
        )
        return jnp.sum(parts.astype(F32), axis=0)

    tokens = gather(mod_in)
    d_tok = gather(d_branch)

    def half_block(up, down):
        pre = dot(tokens, up, ((1,), (0,)))
        hid, back = jax.vjp(gelu_tanh, pre)
        d_hid = dot(d_tok, down, ((1,), (1,)))
        return hid.astype(BF16), back(d_hid)[0].astype(BF16)

    hid_own, dpre_own = half_block(up_own, down_own)
    hid_other, dpre_other = half_block(up_other, down_other)
    branch = scatter(hid_own, hid_other, down_own, down_other, ((1,), (0,)))
    d_mod = scatter(dpre_own, dpre_other, up_own, up_other, ((1,), (1,)))

    up_sent = dot(tokens, dpre_other, ((0,), (0,))).astype(BF16)
    down_sent = dot(hid_other, d_tok, ((0,), (0,))).astype(BF16)
    up_back = swap(up_sent, "dp", dp, 1)
    down_back = swap(down_sent, "dp", dp, 1)
    g_up = dot(tokens, dpre_own, ((0,), (0,))) + up_back.astype(F32)
    g_down = dot(hid_own, d_tok, ((0,), (0,))) + down_back.astype(F32)
    grad_up = (
        lax.all_to_all(g_up.astype(BF16).reshape(dp, d_rows, f), "dp", 0, 0, tiled=True)
        .transpose(1, 0, 2)
        .reshape(d_rows, ff_m)
        .astype(F32)
    )
    grad_down = (
        lax.all_to_all(
            g_down.astype(BF16).reshape(f, dp, d_rows).transpose(1, 0, 2),
            "dp",
            0,
            0,
            tiled=True,
        )
        .reshape(ff_m, d_rows)
        .astype(F32)
    )

    block_out = (joined32 + gate * branch).astype(BF16)
    d_normed = d_mod * (1.0 + scale)
    d_full = d_out32 + inv_std * (
        d_normed
        - jnp.mean(d_normed, axis=-1, keepdims=True)
        - normed * jnp.mean(d_normed * normed, axis=-1, keepdims=True)
    )
    null_part = jnp.where(dropped, d_full[:n_text], F32(0.0)).astype(BF16)
    null_sum = lax.psum(null_part, "dp")

    def whole(rows):
        every = lax.all_gather(rows, "mp", axis=0)
        return jnp.concatenate(
            [
                every[:, :n_text].reshape(-1, width),
                every[:, n_text:].reshape(-1, width),
            ],
            axis=0,
        )[None]

    grad_null = lax.all_gather(null_sum, "mp", axis=0, tiled=True).astype(F32)
    return (whole(block_out), whole(d_full.astype(BF16)), grad_up, grad_down, grad_null)


def solution(mesh):
    placed = (
        P("dp", None, None),
        P("dp", None, None),
        P(),
        P("dp"),
        P("dp"),
        P(),
        P("dp", "mp"),
        P("mp", "dp"),
        P("dp", None, None),
    )
    return jax.shard_map(
        functools.partial(shards, mesh.shape["dp"], mesh.shape["mp"]),
        mesh=mesh,
        in_specs=placed,
        out_specs=(P("dp", None, None), P("dp", None, None), P("dp", "mp"), P("mp", "dp"), P()),
        check_vma=False,
    )
```
